128 devices in a mesh: owner: 8 (over x, core), rows: 16 (over z, y).
Axes of the slice: x: 4, y: 4, z: 4, core: 2. Of those that a mesh axis runs over, the one named last changes fastest.
Arguments:
- train_gate: float32 [128, 2048, 768], P('owner', 'rows'), may hold values from -0.1875 to 0.1875
- train_up: float32 [128, 2048, 768], P('owner', 'rows'), may hold values from -0.1875 to 0.1875
- router_weight: float32 [2048, 128], P('rows', 'owner'), may hold values from -0.125 to 0.125
- router_gain: float32 [2048], P('rows'), may hold values from 0.25 to 1.75
Outputs:
- ready_gate: bfloat16 [128, 2048, 768], P(('owner', 'rows'))
- ready_up: bfloat16 [128, 2048, 768], P(('owner', 'rows'))
- scale_gate: float32 [128, 768], P(('owner', 'rows'))
- scale_up: float32 [128, 768], P(('owner', 'rows'))
- serve_router: bfloat16 [2048, 128], replicated
The draws below stay inside these ranges and needn't reach their ends.
All inputs are finite; a program needn't handle non-finite values.
Results may differ from the reference program's by a relative error of at most 0.001.
Values may be sent and summed in bfloat16 or wider, within the bound.
A program may use at most 128 MiB of HBM per device.

```python
import jax
import jax.numpy as jnp
from jax import lax

EXPERTS = 128
D_MODEL = 2048
D_EXPERT = 768


def spiked(drawn, rng, source, target, parts, factor):
    def block_of(position):
        return (jnp.arange(drawn.shape[position]) // (drawn.shape[position] // parts)).reshape((-1,) + (1,) * (drawn.ndim - 1 - position))

    near = jax.random.permutation(rng, parts)[block_of(target)]
    other_side = (block_of(target) + parts // 2) % parts
    return jnp.where((block_of(source) == near) | (block_of(source) == other_side), factor * drawn, drawn)


def shard_levels(key, dims, cuts, low, high):
    loudness, own = 1.0, jax.random.fold_in(key, 6)
    for axis_at, blocks in cuts:
        heights = jnp.exp(jax.random.uniform(jax.random.fold_in(own, axis_at), (blocks,), jnp.float32, low / len(cuts), high / len(cuts)))
        loudness = loudness * jnp.repeat(heights, dims[axis_at] // blocks).reshape([-1 if axis == axis_at else 1 for axis in range(len(dims))])
    return loudness


def noise(stream_key, extent, spread, most, split=(), dtype=jnp.bfloat16):
    result = jax.random.normal(stream_key, extent, jnp.float32) * spread
    if len(split) > 0:
        result = shard_levels(stream_key, extent, split, -0.22, 0.18) * result
    return jnp.clip(result, min=-most, max=most).astype(dtype)


def heavy_noise(stream_key, extent, spread, reach, pieces, heavy, kind=jnp.bfloat16):
    result = spread * jax.random.normal(stream_key, extent, jnp.float32)
    if pieces:
        result = result * shard_levels(stream_key, extent, pieces, -0.22, 0.18)
    return jnp.clip(spiked(result, jax.random.fold_in(stream_key, 3), *heavy), -reach, reach).astype(kind)


def setup_inputs(seed: int = 0) -> dict:
    splits = jax.random.split(jax.random.key(seed), 5)
    train_gate = heavy_noise(splits[0], (EXPERTS, D_MODEL, D_EXPERT), D_MODEL ** -0.5, 0.1875, ((0, 8), (1, 16)), (1, 2, 16, 2.0), jnp.float32)
    train_up = heavy_noise(splits[1], (EXPERTS, D_MODEL, D_EXPERT), D_MODEL ** -0.5, 0.1875, ((0, 8), (1, 16)), (1, 2, 16, 2.0), jnp.float32)
    router_weight = noise(splits[2], (D_MODEL, EXPERTS), D_MODEL ** -0.5, 0.125, ((0, 16), (1, 8)), jnp.float32)
    router_gain = jnp.clip(1.0 + 0.15 * jax.random.normal(splits[3], (D_MODEL,), jnp.float32), 0.25, 1.75)
    return dict(train_gate=train_gate, train_up=train_up, router_weight=router_weight, router_gain=router_gain)


def reference(train_gate, train_up, router_weight, router_gain):
    scale_gate = jnp.sqrt(lax.optimization_barrier(jnp.sum(train_gate * train_gate, axis=1)))
    ready_gate = (train_gate / jnp.expand_dims(scale_gate, 1)).astype(jnp.bfloat16)
    scale_up = jnp.sqrt(lax.optimization_barrier(jnp.sum(train_up * train_up, axis=1)))
    ready_up = (train_up / jnp.expand_dims(scale_up, 1)).astype(jnp.bfloat16)
    serve_router = (router_weight * router_gain[:, None]).astype(jnp.bfloat16)
    return (ready_gate, ready_up, scale_gate, scale_up, serve_router)
```

```python
import functools

import jax
import jax.numpy as jnp
from jax import lax
from jax.experimental import pallas as pl
from jax.experimental.pallas import tpu as pltpu
from jax.sharding import PartitionSpec as P

MESH = pl.DeviceIdType.MESH
F32, BF16 = jnp.float32, jnp.bfloat16
SIDE = 4
ROWS = SIDE * SIDE
OWNERS = 8
LANES = 128
TILES = 6
EARLY = 2
LATE = TILES - EARLY
REST = LATE + TILES
PART = 2
GROUP = 4


def wrap(k):
    return lax.rem(k * 5, ROWS)


def exchange(
    gate, up, weight, gain,
    land, router, total,
    full, stage, early_y, early_z, late, late_in, late_all, early_total, inverse, late_inverse,
    weight_in, gain_in,
    load_sem, small_sem, y_send, y_recv, z_send, z_recv,
    sum_send, sum_recv, all_send, all_recv,
    data_send, data_recv, plane_send, plane_recv, owner_send, owner_recv,
):
    me = lax.axis_index("rows")
    own = lax.axis_index("owner")
    z, y = me // SIDE, lax.rem(me, SIDE)
    width = PART * LANES

    def rank(k):
        offset = wrap(k)
        to_z = lax.rem(z + offset // SIDE, SIDE)
        return to_z * SIDE + lax.rem(y + lax.rem(offset, SIDE), SIDE)

    def source(k):
        offset = wrap(k)
        from_z = lax.rem(z + SIDE - offset // SIDE, SIDE)
        return from_z * SIDE + lax.rem(y + SIDE - lax.rem(offset, SIDE), SIDE)

    def remote(src, dst, send, recv, **to):
        return pltpu.make_async_remote_copy(
            src_ref=src, dst_ref=dst, send_sem=send, recv_sem=recv,
            device_id=to, device_id_type=MESH,
        )

    loads = []
    early_width = EARLY * LANES
    late_width = LATE * LANES
    for matrix, ref, start, columns in (
        (0, gate, 0, early_width), (0, gate, early_width, late_width), (1, up, 0, TILES * LANES),
    ):
        here = []
        for g in range(ROWS // GROUP):
            part = (pl.ds(g * GROUP, GROUP), slice(None), pl.ds(start, columns))
            copy = pltpu.make_async_copy(
                ref.at[part], full.at[(matrix, *part)], load_sem.at[len(loads), g]
            )
            copy.start()
            here.append(copy)
        loads.append(here)
    weight_copy = pltpu.make_async_copy(weight, weight_in, small_sem.at[0])
    gain_copy = pltpu.make_async_copy(gain, gain_in, small_sem.at[1])
    weight_copy.start()
    gain_copy.start()

    barrier = pltpu.get_barrier_semaphore()
    for k in range(1, ROWS):
        pl.semaphore_signal(barrier, inc=1, device_id={"rows": lax.rem(me + k, ROWS)}, device_id_type=MESH)
    for k in range(1, OWNERS):
        pl.semaphore_signal(barrier, inc=1, device_id={"owner": lax.rem(own + k, OWNERS)}, device_id_type=MESH)

    def squares(matrix, e, tile):
        x = full[matrix, e, :, pl.ds(tile * LANES, LANES)]
        return jnp.sum(x * x, axis=0, keepdims=True)

    late[...] = jnp.zeros_like(late)
    for g in range(ROWS // GROUP):
        loads[0][g].wait()

        @pl.loop(g * GROUP, (g + 1) * GROUP)
        def _(e):
            for t in range(EARLY):
                early_y[y, pl.ds(e * EARLY + t, 1), :] = squares(0, e, t)

    pl.semaphore_wait(barrier, ROWS + OWNERS - 2)

    def across(slots, at, send, recv, axis):
        copies = []
        for d in range(1, SIDE):
            to = lax.rem(at + d, SIDE)
            peer = z * SIDE + to if axis == "y" else to * SIDE + y
            copies.append(remote(slots.at[at], slots.at[at], send.at[d], recv.at[d], rows=peer))
        for copy in copies:
            copy.start()
        return copies

    y_copies = across(early_y, y, y_send, y_recv, "y")

    for g in range(ROWS // GROUP):
        loads[1][g].wait()

        @pl.loop(g * GROUP, (g + 1) * GROUP)
        def _(e):
            for t in range(LATE):
                late[e, pl.ds(t, 1), :] = squares(0, e, EARLY + t)

    for g in range(ROWS // GROUP):
        loads[2][g].wait()

        @pl.loop(g * GROUP, (g + 1) * GROUP)
        def _(e):
            for t in range(TILES):
                late[e, pl.ds(LATE + t, 1), :] = squares(1, e, t)

    weight_copy.wait()
    gain_copy.wait()
    router[own, me] = (weight_in[...] * gain_in[...]).astype(BF16)

    for copy in y_copies:
        copy.wait_recv()
    early_z[z] = ((early_y[0] + early_y[1]) + early_y[2]) + early_y[3]
    z_copies = across(early_z, z, z_send, z_recv, "z")

    @pl.loop(1, ROWS)
    def _(k):
        remote(
            late.at[rank(k)], late_in.at[me], sum_send.at[k], sum_recv.at[k], rows=rank(k)
        ).start()

    late_in[me] = late[me]

    for copy in z_copies:
        copy.wait_recv()
    early = ((early_z[0] + early_z[1]) + early_z[2]) + early_z[3]
    early_total[...] = early
    inverse[...] = 1.0 / jnp.sqrt(early)

    def fill(part, e, write):
        matrix, start = part // (TILES // PART), (part % (TILES // PART)) * PART
        for t in range(PART):
            tile = start + t
            if matrix == 0 and tile < EARLY:
                row = inverse[pl.ds(e * EARLY + tile, 1), :]
            else:
                row = late_inverse[e, pl.ds(tile - EARLY if matrix == 0 else LATE + tile, 1), :]
            columns = pl.ds(tile * LANES, LANES)
            write(matrix, columns, (full[matrix, e, :, columns] * row).astype(BF16))

    def for_partner(k, part):
        to = rank(k)

        def write(matrix, columns, value):
            stage[to, pl.ds(matrix * LANES, LANES), columns] = value

        fill(part, to, write)

    def send(k, part):
        matrix, start = part // (TILES // PART), (part % (TILES // PART)) * width
        to = rank(k)
        piece = (pl.ds(matrix * LANES, LANES), pl.ds(start, width))
        remote(
            stage.at[(to, *piece)], land.at[(me, *piece)], data_send.at[k], data_recv.at[k], rows=to
        ).start()

    def batch(part, first, last):
        for_partner(first, part)

        @pl.loop(first + 1, last)
        def _(k):
            for_partner(k, part)
            send(k - 1, part)

        send(last - 1, part)

    def for_self(part):
        def write(matrix, columns, value):
            land[me, pl.ds(matrix * LANES, LANES), columns] = value

        fill(part, me, write)

    batch(0, 1, ROWS // 2)

    @pl.loop(1, ROWS)
    def _(k):
        remote(
            late.at[rank(k)], late_in.at[source(k)], sum_send.at[k], sum_recv.at[k], rows=rank(k)
        ).wait_recv()

    whole = late_in[0]
    for r in range(1, ROWS):
        whole = whole + late_in[r]
    late_all[me] = whole

    @pl.loop(1, ROWS)
    def _(k):
        remote(late_all.at[me], late_all.at[me], all_send.at[k], all_recv.at[k], rows=rank(k)).start()

    batch(0, ROWS // 2, ROWS)
    for_self(0)

    @pl.loop(1, ROWS)
    def _(k):
        remote(
            router.at[own, me], router.at[own, me], plane_send.at[k], plane_recv.at[k], rows=rank(k)
        ).start()

    for t in range(EARLY):
        total[t] = early_total[pl.ds(me * EARLY + t, 1), :]
    for t in range(REST):
        total[EARLY + t] = late_all[me, pl.ds(t, 1), :]

    @pl.loop(1, ROWS)
    def _(k):
        remote(
            late_all.at[me], late_all.at[source(k)], all_send.at[k], all_recv.at[k], rows=rank(k)
        ).wait_recv()

    late_inverse[...] = 1.0 / jnp.sqrt(late_all[...])

    for part in range(1, 2 * TILES // PART):
        batch(part, 1, ROWS)
        for_self(part)
        if part == 1:
            @pl.loop(1, ROWS)
            def _(k):
                remote(
                    router.at[own, me], router.at[own, source(k)], plane_send.at[k], plane_recv.at[k], rows=rank(k)
                ).wait_recv()

            for k in range(1, OWNERS):
                remote(
                    router.at[own], router.at[own], owner_send.at[k], owner_recv.at[k],
                    owner=lax.rem(own + k, OWNERS),
                ).start()

    for copy in y_copies + z_copies:
        copy.wait_send()

    @pl.loop(1, ROWS)
    def _(k):
        to = rank(k)
        remote(late.at[to], late_in.at[me], sum_send.at[k], sum_recv.at[k], rows=to).wait_send()
        remote(late_all.at[me], late_all.at[me], all_send.at[k], all_recv.at[k], rows=to).wait_send()
        remote(router.at[own, me], router.at[own, me], plane_send.at[k], plane_recv.at[k], rows=to).wait_send()

    for k in range(1, OWNERS):
        copy = remote(
            router.at[own], router.at[lax.rem(own + OWNERS - k, OWNERS)], owner_send.at[k], owner_recv.at[k],
            owner=lax.rem(own + k, OWNERS),
        )
        copy.wait_send()
        copy.wait_recv()

    @pl.loop(1, ROWS)
    def _(k):
        copy = remote(stage.at[rank(k)], land.at[source(k)], data_send.at[k], data_recv.at[k], rows=rank(k))
        copy.wait_send()
        copy.wait_recv()


def lay_out(land, router, total, gate, up, scale_gate, scale_up, serve, sem):
    copies = []
    for half in range(2):
        for matrix, out in ((0, gate), (1, up)):
            some = pl.ds(half * ROWS // 2, ROWS // 2)
            copy = pltpu.make_async_copy(
                land.at[some, pl.ds(matrix * LANES, LANES)], out.at[some], sem.at[half, matrix]
            )
            copy.start()
            copies.append(copy)
    for t in range(TILES):
        columns = slice(t * LANES, (t + 1) * LANES)
        scale_gate[:, columns] = jnp.sqrt(total[t])
        scale_up[:, columns] = jnp.sqrt(total[TILES + t])
    for r in range(ROWS):
        block = jnp.concatenate([router[o, r] for o in range(OWNERS)], axis=0).astype(F32)
        serve[r * LANES:(r + 1) * LANES, :] = block.T.astype(BF16)
    for copy in copies:
        copy.wait()


def on_device(gate, up, weight, gain):
    hbm = pl.BlockSpec(memory_space=pltpu.HBM)
    vmem = pl.BlockSpec(memory_space=pltpu.VMEM)
    experts, rows, columns = gate.shape
    dma = pltpu.SemaphoreType.DMA
    land, router, total = pl.pallas_call(
        exchange,
        name="exchange",
        out_shape=(
            jax.ShapeDtypeStruct((ROWS, 2 * rows, columns), BF16),
            jax.ShapeDtypeStruct((OWNERS, ROWS, LANES // OWNERS, rows), BF16),
            jax.ShapeDtypeStruct((2 * TILES, 1, LANES), F32),
        ),
        in_specs=[hbm] * 4,
        out_specs=(vmem,) * 3,
        scratch_shapes=[
            pltpu.VMEM((2, experts, rows, columns), F32),
            pltpu.VMEM((ROWS, 2 * rows, columns), BF16),
            pltpu.VMEM((SIDE, experts * EARLY, LANES), F32),
            pltpu.VMEM((SIDE, experts * EARLY, LANES), F32),
            pltpu.VMEM((experts, 16, LANES), F32),
            pltpu.VMEM((experts, 16, LANES), F32),
            pltpu.VMEM((experts, 16, LANES), F32),
            pltpu.VMEM((experts * EARLY, LANES), F32),
            pltpu.VMEM((experts * EARLY, LANES), F32),
            pltpu.VMEM((experts, 16, LANES), F32),
            pltpu.VMEM((LANES // OWNERS, rows), F32),
            pltpu.VMEM((1, rows), F32),
            dma((3, ROWS // GROUP)),
            dma((2,)),
            dma((SIDE,)), dma((SIDE,)), dma((SIDE,)), dma((SIDE,)),
            dma((ROWS,)), dma((ROWS,)), dma((ROWS,)), dma((ROWS,)),
            dma((ROWS,)), dma((ROWS,)), dma((ROWS,)), dma((ROWS,)),
            dma((OWNERS,)), dma((OWNERS,)),
        ],
        compiler_params=pltpu.CompilerParams(
            collective_id=0, has_side_effects=True, vmem_limit_bytes=36 << 20
        ),
    )(*(pltpu.with_memory_space_constraint(a, pltpu.HBM) for a in (gate, up, weight.T, gain.reshape(1, rows))))
    ready = jax.ShapeDtypeStruct((ROWS, rows, columns), BF16)
    scale = jax.ShapeDtypeStruct((1, columns), F32)
    ready_gate, ready_up, scale_gate, scale_up, serve = pl.pallas_call(
        lay_out,
        name="lay_out",
        out_shape=(ready, ready, scale, scale, jax.ShapeDtypeStruct((ROWS * rows, LANES), BF16)),
        in_specs=[vmem] * 3,
        out_specs=(hbm, hbm, vmem, vmem, vmem),
        scratch_shapes=[dma((2, 2))],
        compiler_params=pltpu.CompilerParams(vmem_limit_bytes=16 << 20),
    )(land, router, total)
    whole = (1, ROWS * rows, columns)
    return ready_gate.reshape(whole), ready_up.reshape(whole), scale_gate, scale_up, serve


def solution(mesh):
    return jax.shard_map(
        on_device,
        mesh=mesh,
        in_specs=(P("owner", "rows", None), P("owner", "rows", None), P("rows", "owner"), P("rows")),
        out_specs=(
            P(("owner", "rows"), None, None),
            P(("owner", "rows"), None, None),
            P(("owner", "rows"), None),
            P(("owner", "rows"), None),
            P(),
        ),
        check_vma=False,
    )
```

```python
import jax
import jax.numpy as jnp
from jax import lax
from jax.experimental import pallas as pl
from jax.experimental.pallas import tpu as pltpu
from jax.sharding import PartitionSpec as P

MESH = pl.DeviceIdType.MESH
F32, BF16 = jnp.float32, jnp.bfloat16
SIDE = 4
ROWS = SIDE * SIDE
OWNERS = 8
LANES = 128
DEEP = 128
TILES = 6
PART = 2
PARTS = TILES // PART
FIRST = 2
EARLY = FIRST * PART
LATE = 2 * TILES - EARLY
GROUP = 4
RAW = 32
HALF = RAW // 2
ORDER = (
    (2, 2), (3, 2), (2, 3), (1, 2), (2, 1), (2, 0), (0, 2), (3, 1), (1, 3), (3, 3), (1, 1), (1, 0), (0, 3), (3, 0), (0, 1),
)
NEAR = tuple(step for step in ORDER if 0 in step)


def exchange(
    gate, up, weight, gain,
    land, serve, scale_gate, scale_up,
    full, stage, raw, router, early_y, early_z, early_total,
    late, late_y, late_sum, late_z, late_all, inverse, weight_in, gain_in,
    load_sem, small_sem, y_send, y_recv, z_send, z_recv, raw_send, raw_recv,
    late_y_send, late_y_recv, late_z_send, late_z_recv, all_send, all_recv,
    data_send, data_recv, plane_send, plane_recv, owner_send, owner_recv,
):
    me = lax.axis_index("rows")
    own = lax.axis_index("owner")
    z, y = me // SIDE, lax.rem(me, SIDE)
    width = PART * LANES

    def shifted(step):
        return lax.rem(z + step[0], SIDE) * SIDE + lax.rem(y + step[1], SIDE)

    def back(step):
        return shifted((SIDE - step[0], SIDE - step[1]))

    def slot(step):
        return step[0] * SIDE + step[1]

    def remote(src, dst, send, recv, **to):
        return pltpu.make_async_remote_copy(
            src_ref=src, dst_ref=dst, send_sem=send, recv_sem=recv,
            device_id=to, device_id_type=MESH,
        )

    loads = []
    for matrix, ref, start, tiles in (
        (0, gate, 0, PART), (0, gate, PART, EARLY - PART), (0, gate, EARLY, TILES - EARLY), (1, up, 0, TILES),
    ):
        here = []
        for g in range(ROWS // GROUP):
            part = (pl.ds(g * GROUP, GROUP), slice(None), pl.ds(start * LANES, tiles * LANES))
            copy = pltpu.make_async_copy(
                ref.at[part], full.at[(matrix, *part)], load_sem.at[len(loads), g]
            )
            copy.start()
            here.append(copy)
        loads.append(here)
    weight_copy = pltpu.make_async_copy(weight, weight_in, small_sem.at[0])
    gain_copy = pltpu.make_async_copy(gain, gain_in, small_sem.at[1])
    weight_copy.start()
    gain_copy.start()

    barrier = pltpu.get_barrier_semaphore()
    for step in NEAR:
        pl.semaphore_signal(barrier, inc=1, device_id={"rows": shifted(step)}, device_id_type=MESH)
    for d in range(1, OWNERS):
        pl.semaphore_signal(barrier, inc=1, device_id={"owner": lax.rem(own + d, OWNERS)}, device_id_type=MESH)

    def squares(matrix, e, tile):
        x = full[matrix, e, :, pl.ds(tile * LANES, LANES)]
        return jnp.sum(x * x, axis=0, keepdims=True)

    def early_squares(i):
        for g in range(ROWS // GROUP):
            loads[i][g].wait()

            @pl.loop(g * GROUP, (g + 1) * GROUP)
            def _(e):
                for t in range(PART):
                    early_y[i, y, e, t] = squares(0, e, i * PART + t)

    early_squares(0)
    pl.semaphore_wait(barrier, len(NEAR) + OWNERS - 1)

    def across(source, slots, at, send, recv, along_z):
        copies = []
        for d in (2, 1, 3):
            to = lax.rem((z if along_z else y) + d, SIDE)
            peer = shifted((d, 0) if along_z else (0, d))
            copies.append(remote(source(to), slots.at[at], send.at[d], recv.at[d], rows=peer))
            copies[-1].start()
        return copies

    def raw_copy(i, half):
        to = shifted(NEAR[i])
        return remote(
            up.at[to, pl.ds(DEEP - RAW + half * HALF, HALF)], raw.at[i, pl.ds(half * HALF, HALF)],
            raw_send.at[i, half], raw_recv.at[i, half], rows=to,
        )

    def early_across(i, slots, at, send, recv, along_z):
        return across(lambda to: slots.at[i, at], slots.at[i], at, send.at[i], recv.at[i], along_z)

    def taken(slots):
        return ((slots[0] + slots[1]) + slots[2]) + slots[3]

    y_copies = [early_across(0, early_y, y, y_send, y_recv, False)]
    if RAW:
        for i in range(len(NEAR)):
            raw_copy(i, 0).start()

    def late_squares(matrix, start, loaded):
        for g in range(ROWS // GROUP):
            loaded[g].wait()

            @pl.loop(g * GROUP, (g + 1) * GROUP)
            def _(e):
                for t in range(start, TILES):
                    late[lax.rem(e, SIDE), e // SIDE, matrix * TILES + t - EARLY] = squares(matrix, e, t)

    for i in range(1, FIRST):
        early_squares(i)
        y_copies.append(early_across(i, early_y, y, y_send, y_recv, False))
    late_squares(0, EARLY, loads[2])
    late_squares(1, 0, loads[3])
    late_y_copies = across(lambda to: late.at[to], late_y, y, late_y_send, late_y_recv, False)

    weight_copy.wait()
    gain_copy.wait()
    router[own, me] = (weight_in[...] * gain_in[...]).astype(BF16)
    late_y[y] = late[y]

    z_copies = []
    for i in range(FIRST):
        for copy in y_copies[i]:
            copy.wait_recv()
        early_z[i, z] = taken(early_y.at[i])
        z_copies.append(early_across(i, early_z, z, z_send, z_recv, True))
        if RAW and i == 0:
            for j in range(len(NEAR)):
                raw_copy(j, 1).start()

    for copy in late_y_copies:
        copy.wait_recv()
    late_sum[...] = taken(late_y)
    late_z[z] = late_sum[z]
    late_z_copies = across(lambda to: late_sum.at[to], late_z, z, late_z_send, late_z_recv, True)

    def early_whole(i):
        for copy in z_copies[i]:
            copy.wait_recv()
        whole = taken(early_z.at[i])
        early_total[:, i * PART:(i + 1) * PART] = whole
        inverse[:, i * PART:(i + 1) * PART] = 1.0 / jnp.sqrt(whole)

    def fill(part, e, deep, write):
        matrix, start = part // PARTS, lax.rem(part, PARTS) * PART
        for t in range(PART):
            columns = pl.ds(pl.multiple_of((start + t) * LANES, LANES), LANES)
            row = inverse[e, part * PART + t]
            value = (full[matrix, e, pl.ds(0, deep), columns] * row).astype(BF16)
            write(pl.ds(pl.multiple_of(matrix * DEEP, DEEP), deep), columns, value)

    def prepare(step, part, deep):
        to = shifted(step)

        def write(rows, columns, value):
            stage[to, rows, columns] = value

        fill(part, to, deep, write)

    def send(step, part, deep):
        piece = (
            pl.ds(pl.multiple_of(part // PARTS * DEEP, DEEP), deep),
            pl.ds(pl.multiple_of(lax.rem(part, PARTS) * width, width), width),
        )
        k = slot(step)
        to = shifted(step)
        remote(
            stage.at[(to, *piece)], land.at[(me, *piece)], data_send.at[k], data_recv.at[k], rows=to
        ).start()

    def batch(part, steps, less=0):
        waiting = None
        for step in steps:
            deep = DEEP - (less if step in NEAR else 0)
            prepare(step, part, deep)
            if waiting:
                send(waiting[0], part, waiting[1])
            waiting = step, deep
        send(waiting[0], part, waiting[1])

    def for_self(part):
        def write(rows, columns, value):
            land[me, rows, columns] = value

        fill(part, me, DEEP, write)

    early_whole(0)
    batch(0, ORDER)

    for copy in late_z_copies:
        copy.wait_recv()
    late_all[me] = taken(late_z)

    def all_copy(step, at):
        return remote(
            late_all.at[me], late_all.at[at], all_send.at[slot(step)], all_recv.at[slot(step)], rows=shifted(step)
        )

    for_self(0)
    for step in ORDER:
        all_copy(step, me).start()

    for part in range(1, FIRST):
        early_whole(part)
        batch(part, ORDER)

    def plane_copy(step, at):
        return remote(
            router.at[own, me], router.at[own, at], plane_send.at[slot(step)], plane_recv.at[slot(step)],
            rows=shifted(step),
        )

    for step in ORDER:
        plane_copy(step, me).start()

    for t in range(TILES):
        columns = pl.ds(t * LANES, LANES)
        scale_gate[:, columns] = jnp.sqrt(early_total[me, t] if t < EARLY else late_all[me, t - EARLY])
        scale_up[:, columns] = jnp.sqrt(late_all[me, TILES + t - EARLY])

    for step in ORDER:
        all_copy(step, back(step)).wait_recv()
    inverse[:, EARLY:] = 1.0 / jnp.sqrt(late_all[...])

    for part in range(FIRST, PARTS):
        batch(part, ORDER)

    @pl.loop(PARTS, 2 * PARTS)
    def _(part):
        batch(part, ORDER, RAW)

    @pl.loop(1, 2 * PARTS)
    def _(part):
        for_self(part)

    for step in ORDER:
        plane_copy(step, back(step)).wait_recv()

    def owner_copy(d, at):
        return remote(
            router.at[own], router.at[at], owner_send.at[d], owner_recv.at[d], owner=lax.rem(own + d, OWNERS)
        )

    for d in range(1, OWNERS):
        owner_copy(d, own).start()

    if RAW:
        for i, step in enumerate(NEAR):
            for half in range(2):
                raw_copy(i, half).wait_recv()
            for t in range(TILES):
                columns = pl.ds(t * LANES, LANES)
                land[back(step), pl.ds(2 * DEEP - RAW, RAW), columns] = (
                    raw[i, :, columns] * inverse[me, TILES + t]
                ).astype(BF16)

    for d in range(1, OWNERS):
        owner_copy(d, lax.rem(own + OWNERS - d, OWNERS)).wait_recv()
    for r in range(ROWS):
        block = jnp.concatenate([router[o, r] for o in range(OWNERS)], axis=0).astype(F32)
        serve[r * DEEP:(r + 1) * DEEP, :] = block.T.astype(BF16)

    for copy in sum(y_copies + z_copies, []) + late_y_copies + late_z_copies:
        copy.wait_send()
    if RAW:
        for i in range(len(NEAR)):
            for half in range(2):
                raw_copy(i, half).wait_send()
    for d in range(1, OWNERS):
        owner_copy(d, own).wait_send()
    for step in ORDER:
        all_copy(step, me).wait_send()
        plane_copy(step, me).wait_send()
    for step in ORDER:
        rows = pl.ds(0, 2 * DEEP - (RAW if step in NEAR else 0))
        k = slot(step)
        copy = remote(
            stage.at[shifted(step), rows], land.at[back(step), rows], data_send.at[k], data_recv.at[k],
            rows=shifted(step),
        )
        copy.wait_send()
        copy.wait_recv()


def lay_out(land, serve, scale_gate, scale_up, gate_out, up_out, serve_out, scale_gate_out, scale_up_out, sem):
    copies = [
        (land.at[:, pl.ds(0, DEEP)], gate_out),
        (land.at[:, pl.ds(DEEP, DEEP)], up_out),
        (serve, serve_out),
        (scale_gate, scale_gate_out),
        (scale_up, scale_up_out),
    ]
    copies = [pltpu.make_async_copy(src, dst, sem.at[i]) for i, (src, dst) in enumerate(copies)]
    for copy in copies:
        copy.start()
    for copy in copies:
        copy.wait()


def on_device(gate, up, weight, gain):
    hbm = pl.BlockSpec(memory_space=pltpu.HBM)
    vmem = pl.BlockSpec(memory_space=pltpu.VMEM)
    experts, rows, columns = gate.shape
    dma = pltpu.SemaphoreType.DMA
    scale = jax.ShapeDtypeStruct((1, columns), F32)
    router = jax.ShapeDtypeStruct((ROWS * rows, LANES), BF16)
    inputs = (gate, up, weight.T, gain.reshape(1, rows))
    sums = lambda *lead: pltpu.VMEM((*lead, 1, LANES), F32)
    done = pl.pallas_call(
        exchange,
        name="exchange",
        out_shape=(jax.ShapeDtypeStruct((ROWS, 2 * rows, columns), BF16), router, scale, scale),
        in_specs=[hbm] * 4,
        out_specs=(vmem,) * 4,
        scratch_shapes=[
            pltpu.VMEM((2, experts, rows, columns), F32),
            pltpu.VMEM((ROWS, 2 * rows, columns), BF16),
            pltpu.VMEM((len(NEAR), max(RAW, 8), columns), F32),
            pltpu.VMEM((OWNERS, ROWS, LANES // OWNERS, rows), BF16),
            sums(FIRST, SIDE, experts, PART),
            sums(FIRST, SIDE, experts, PART),
            sums(experts, EARLY),
            sums(SIDE, SIDE, LATE),
            sums(SIDE, SIDE, LATE),
            sums(SIDE, LATE),
            sums(SIDE, LATE),
            sums(experts, LATE),
            sums(experts, 2 * TILES),
            pltpu.VMEM((LANES // OWNERS, rows), F32),
            pltpu.VMEM((1, rows), F32),
            dma((4, ROWS // GROUP)),
            dma((2,)),
            dma((FIRST, SIDE)), dma((FIRST, SIDE)), dma((FIRST, SIDE)), dma((FIRST, SIDE)),
            dma((len(NEAR), 2)), dma((len(NEAR), 2)),
            dma((SIDE,)), dma((SIDE,)), dma((SIDE,)), dma((SIDE,)),
            dma((ROWS,)), dma((ROWS,)), dma((ROWS,)), dma((ROWS,)),
            dma((ROWS,)), dma((ROWS,)),
            dma((OWNERS,)), dma((OWNERS,)),
        ],
        compiler_params=pltpu.CompilerParams(
            collective_id=0, has_side_effects=True, vmem_limit_bytes=36 << 20
        ),
    )(*(pltpu.with_memory_space_constraint(a, pltpu.HBM) for a in inputs))
    ready = jax.ShapeDtypeStruct((ROWS, rows, columns), BF16)
    ready_gate, ready_up, serve, scale_gate, scale_up = pl.pallas_call(
        lay_out,
        name="lay_out",
        out_shape=(ready, ready, router, scale, scale),
        in_specs=[vmem] * 4,
        out_specs=(hbm,) * 5,
        scratch_shapes=[dma((5,))],
        compiler_params=pltpu.CompilerParams(vmem_limit_bytes=8 << 20),
    )(*done)
    whole = (1, ROWS * rows, columns)
    return ready_gate.reshape(whole), ready_up.reshape(whole), scale_gate, scale_up, serve


def solution(mesh):
    return jax.shard_map(
        on_device,
        mesh=mesh,
        in_specs=(P("owner", "rows", None), P("owner", "rows", None), P("rows", "owner"), P("rows")),
        out_specs=(
            P(("owner", "rows"), None, None),
            P(("owner", "rows"), None, None),
            P(("owner", "rows"), None),
            P(("owner", "rows"), None),
            P(),
        ),
        check_vma=False,
    )
```

```python
import jax
import jax.numpy as jnp
from jax import lax
from jax.experimental import pallas as pl
from jax.experimental.pallas import tpu as pltpu
from jax.sharding import PartitionSpec as P

MESH = pl.DeviceIdType.MESH
F32, BF16 = jnp.float32, jnp.bfloat16
SIDE = 4
ROWS = SIDE * SIDE
OWNERS = 8
LANES = 128
DEEP = 128
TILES = 6
PART = 2
EAGER = ((0, 1), (1, 2))
EARLY = 3
LATE = 2 * TILES - EARLY
GROUP = 4
RAW = 24
HALF = 16
ORDER = (
    (1, 2), (2, 3), (2, 0), (3, 1), (2, 1), (0, 2), (3, 3), (1, 1), (2, 2), (3, 2), (1, 3), (0, 3), (1, 0), (3, 0), (0, 1),
)
NEAR = tuple(step for step in ORDER if 0 in step)


def exchange(
    gate, up, weight, gain,
    land, serve, scale_gate, scale_up,
    full, stage, raw, router, early_y_0, early_y_1, early_z_0, early_z_1, early_total,
    late, late_y, late_sum, late_z, late_all, inverse, weight_in, gain_in,
    load_sem, small_sem, y_send, y_recv, z_send, z_recv, raw_send, raw_recv,
    late_y_send, late_y_recv, late_z_send, late_z_recv, all_send, all_recv,
    data_send, data_recv, plane_send, plane_recv, owner_send, owner_recv,
):
    me = lax.axis_index("rows")
    own = lax.axis_index("owner")
    z, y = me // SIDE, lax.rem(me, SIDE)

    def shifted(step):
        return lax.rem(z + step[0], SIDE) * SIDE + lax.rem(y + step[1], SIDE)

    def back(step):
        return shifted((SIDE - step[0], SIDE - step[1]))

    def slot(step):
        return step[0] * SIDE + step[1]

    def remote(src, dst, send, recv, **to):
        return pltpu.make_async_remote_copy(
            src_ref=src, dst_ref=dst, send_sem=send, recv_sem=recv,
            device_id=to, device_id_type=MESH,
        )

    loads = []
    for matrix, ref, start, tiles in (
        *((0, gate, *tiles) for tiles in EAGER), (0, gate, EARLY, TILES - EARLY), (1, up, 0, TILES),
    ):
        here = []
        for g in range(ROWS // GROUP):
            part = (pl.ds(g * GROUP, GROUP), slice(None), pl.ds(start * LANES, tiles * LANES))
            copy = pltpu.make_async_copy(
                ref.at[part], full.at[(matrix, *part)], load_sem.at[len(loads), g]
            )
            copy.start()
            here.append(copy)
        loads.append(here)
    weight_copy = pltpu.make_async_copy(weight, weight_in, small_sem.at[0])
    gain_copy = pltpu.make_async_copy(gain, gain_in, small_sem.at[1])
    weight_copy.start()
    gain_copy.start()

    barrier = pltpu.get_barrier_semaphore()
    for step in NEAR:
        pl.semaphore_signal(barrier, inc=1, device_id={"rows": shifted(step)}, device_id_type=MESH)
    for d in range(1, OWNERS):
        pl.semaphore_signal(barrier, inc=1, device_id={"owner": lax.rem(own + d, OWNERS)}, device_id_type=MESH)

    early_y, early_z = (early_y_0, early_y_1), (early_z_0, early_z_1)

    def squares(matrix, e, tile):
        x = full[matrix, e, :, pl.ds(tile * LANES, LANES)]
        return jnp.sum(x * x, axis=0, keepdims=True)

    def early_squares(i):
        for g in range(ROWS // GROUP):
            loads[i][g].wait()

            @pl.loop(g * GROUP, (g + 1) * GROUP)
            def _(e):
                for t in range(EAGER[i][1]):
                    early_y[i][y, e, t] = squares(0, e, EAGER[i][0] + t)

    early_squares(0)
    pl.semaphore_wait(barrier, len(NEAR) + OWNERS - 1)

    def across(source, slots, at, send, recv, along_z):
        copies = []
        for d in (2, 1, 3):
            to = lax.rem((z if along_z else y) + d, SIDE)
            peer = shifted((d, 0) if along_z else (0, d))
            copies.append(remote(source(to), slots.at[at], send.at[d], recv.at[d], rows=peer))
            copies[-1].start()
        return copies

    def raw_copy(i, half):
        to = shifted(NEAR[i])
        return remote(
            up.at[to, pl.ds(DEEP - RAW + half * HALF, HALF if half == 0 else RAW - HALF)], raw.at[i, pl.ds(half * HALF, HALF if half == 0 else RAW - HALF)],
            raw_send.at[i, half], raw_recv.at[i, half], rows=to,
        )

    def early_across(i, slots, at, send, recv, along_z):
        return across(lambda to: slots[i].at[at], slots[i], at, send.at[i], recv.at[i], along_z)

    def taken(slots):
        return ((slots[0] + slots[1]) + slots[2]) + slots[3]

    y_copies = [early_across(0, early_y, y, y_send, y_recv, False)]
    if RAW:
        for i in range(len(NEAR)):
            raw_copy(i, 0).start()

    def late_squares(matrix, start, loaded):
        for g in range(ROWS // GROUP):
            loaded[g].wait()

            @pl.loop(g * GROUP, (g + 1) * GROUP)
            def _(e):
                for t in range(start, TILES):
                    late[lax.rem(e, SIDE), e // SIDE, matrix * TILES + t - EARLY] = squares(matrix, e, t)

    for i in range(1, len(EAGER)):
        early_squares(i)
        y_copies.append(early_across(i, early_y, y, y_send, y_recv, False))
    late_squares(0, EARLY, loads[2])
    late_squares(1, 0, loads[3])
    late_y_copies = across(lambda to: late.at[to], late_y, y, late_y_send, late_y_recv, False)

    weight_copy.wait()
    gain_copy.wait()
    router[own, me] = (weight_in[...] * gain_in[...]).astype(BF16)
    late_y[y] = late[y]

    z_copies = []
    for i in range(len(EAGER)):
        for copy in y_copies[i]:
            copy.wait_recv()
        early_z[i][z] = taken(early_y[i])
        z_copies.append(early_across(i, early_z, z, z_send, z_recv, True))
        if RAW and i == 0:
            for j in range(len(NEAR)):
                raw_copy(j, 1).start()

    for copy in late_y_copies:
        copy.wait_recv()
    late_sum[...] = taken(late_y)
    late_z[z] = late_sum[z]
    late_z_copies = across(lambda to: late_sum.at[to], late_z, z, late_z_send, late_z_recv, True)

    def early_whole(i):
        for copy in z_copies[i]:
            copy.wait_recv()
        whole = taken(early_z[i])
        start, count = EAGER[i]
        early_total[:, start:start + count] = whole
        inverse[:, start:start + count] = 1.0 / jnp.sqrt(whole)

    def fill(message, e, deep, write):
        matrix, start, count = message
        for t in range(count):
            columns = pl.ds(pl.multiple_of((start + t) * LANES, LANES), LANES)
            row = inverse[e, matrix * TILES + start + t]
            value = (full[matrix, e, pl.ds(0, deep), columns] * row).astype(BF16)
            write(pl.ds(matrix * DEEP, deep), columns, value)

    def prepare(step, message, deep):
        to = shifted(step)

        def write(rows, columns, value):
            stage[to, rows, columns] = value

        fill(message, to, deep, write)

    def send(step, message, deep):
        matrix, start, count = message
        piece = (pl.ds(matrix * DEEP, deep), pl.ds(pl.multiple_of(start * LANES, LANES), count * LANES))
        k = slot(step)
        to = shifted(step)
        remote(
            stage.at[(to, *piece)], land.at[(me, *piece)], data_send.at[k], data_recv.at[k], rows=to
        ).start()

    def batch(message, less=0):
        waiting = None
        for step in ORDER:
            deep = DEEP - (less if step in NEAR else 0)
            prepare(step, message, deep)
            if waiting:
                send(waiting[0], message, waiting[1])
            waiting = step, deep
        send(waiting[0], message, waiting[1])

    def for_self(message):
        def write(rows, columns, value):
            land[me, rows, columns] = value

        fill(message, me, DEEP, write)

    early_whole(0)
    batch((0, *EAGER[0]))

    for copy in late_z_copies:
        copy.wait_recv()
    late_all[me] = taken(late_z)

    def all_copy(step, at):
        return remote(
            late_all.at[me], late_all.at[at], all_send.at[slot(step)], all_recv.at[slot(step)], rows=shifted(step)
        )

    for step in ORDER:
        all_copy(step, me).start()

    for i in range(1, len(EAGER)):
        early_whole(i)
        batch((0, *EAGER[i]))

    def plane_copy(step, at):
        return remote(
            router.at[own, me], router.at[own, at], plane_send.at[slot(step)], plane_recv.at[slot(step)],
            rows=shifted(step),
        )

    for step in ORDER:
        plane_copy(step, me).start()

    for t in range(TILES):
        columns = pl.ds(t * LANES, LANES)
        scale_gate[:, columns] = jnp.sqrt(early_total[me, t] if t < EARLY else late_all[me, t - EARLY])
        scale_up[:, columns] = jnp.sqrt(late_all[me, TILES + t - EARLY])

    for step in ORDER:
        all_copy(step, back(step)).wait_recv()
    inverse[:, EARLY:] = 1.0 / jnp.sqrt(late_all[...])

    batch((0, EARLY, TILES - EARLY))

    @pl.loop(0, TILES // PART)
    def _(part):
        batch((1, part * PART, PART), RAW)

    for_self((0, 0, TILES))
    for_self((1, 0, TILES))

    for step in ORDER:
        plane_copy(step, back(step)).wait_recv()

    def owner_copy(d, at):
        return remote(
            router.at[own], router.at[at], owner_send.at[d], owner_recv.at[d], owner=lax.rem(own + d, OWNERS)
        )

    for d in range(1, OWNERS):
        owner_copy(d, own).start()

    if RAW:
        for i, step in enumerate(NEAR):
            for half in range(2):
                raw_copy(i, half).wait_recv()
            for t in range(TILES):
                columns = pl.ds(t * LANES, LANES)
                land[back(step), pl.ds(2 * DEEP - RAW, RAW), columns] = (
                    raw[i, :, columns] * inverse[me, TILES + t]
                ).astype(BF16)

    for d in range(1, OWNERS):
        owner_copy(d, lax.rem(own + OWNERS - d, OWNERS)).wait_recv()
    for r in range(ROWS):
        block = jnp.concatenate([router[o, r] for o in range(OWNERS)], axis=0).astype(F32)
        serve[r * DEEP:(r + 1) * DEEP, :] = block.T.astype(BF16)

    for copy in sum(y_copies + z_copies, []) + late_y_copies + late_z_copies:
        copy.wait_send()
    if RAW:
        for i in range(len(NEAR)):
            for half in range(2):
                raw_copy(i, half).wait_send()
    for d in range(1, OWNERS):
        owner_copy(d, own).wait_send()
    for step in ORDER:
        all_copy(step, me).wait_send()
        plane_copy(step, me).wait_send()
    for step in ORDER:
        rows = pl.ds(0, 2 * DEEP - (RAW if step in NEAR else 0))
        k = slot(step)
        copy = remote(
            stage.at[shifted(step), rows], land.at[back(step), rows], data_send.at[k], data_recv.at[k],
            rows=shifted(step),
        )
        copy.wait_send()
        copy.wait_recv()


def lay_out(land, serve, scale_gate, scale_up, gate_out, up_out, serve_out, scale_gate_out, scale_up_out, sem):
    copies = [
        (land.at[:, pl.ds(0, DEEP)], gate_out),
        (land.at[:, pl.ds(DEEP, DEEP)], up_out),
        (serve, serve_out),
        (scale_gate, scale_gate_out),
        (scale_up, scale_up_out),
    ]
    copies = [pltpu.make_async_copy(src, dst, sem.at[i]) for i, (src, dst) in enumerate(copies)]
    for copy in copies:
        copy.start()
    for copy in copies:
        copy.wait()


def on_device(gate, up, weight, gain):
    hbm = pl.BlockSpec(memory_space=pltpu.HBM)
    vmem = pl.BlockSpec(memory_space=pltpu.VMEM)
    experts, rows, columns = gate.shape
    dma = pltpu.SemaphoreType.DMA
    scale = jax.ShapeDtypeStruct((1, columns), F32)
    router = jax.ShapeDtypeStruct((ROWS * rows, LANES), BF16)
    inputs = (gate, up, weight.T, gain.reshape(1, rows))
    sums = lambda *lead: pltpu.VMEM((*lead, 1, LANES), F32)
    done = pl.pallas_call(
        exchange,
        name="exchange",
        out_shape=(jax.ShapeDtypeStruct((ROWS, 2 * rows, columns), BF16), router, scale, scale),
        in_specs=[hbm] * 4,
        out_specs=(vmem,) * 4,
        scratch_shapes=[
            pltpu.VMEM((2, experts, rows, columns), F32),
            pltpu.VMEM((ROWS, 2 * rows, columns), BF16),
            pltpu.VMEM((len(NEAR), max(RAW, 8), columns), F32),
            pltpu.VMEM((OWNERS, ROWS, LANES // OWNERS, rows), BF16),
            *(sums(SIDE, experts, count) for _, count in EAGER * 2),
            sums(experts, EARLY),
            sums(SIDE, SIDE, LATE),
            sums(SIDE, SIDE, LATE),
            sums(SIDE, LATE),
            sums(SIDE, LATE),
            sums(experts, LATE),
            sums(experts, 2 * TILES),
            pltpu.VMEM((LANES // OWNERS, rows), F32),
            pltpu.VMEM((1, rows), F32),
            dma((4, ROWS // GROUP)),
            dma((2,)),
            dma((len(EAGER), SIDE)), dma((len(EAGER), SIDE)), dma((len(EAGER), SIDE)), dma((len(EAGER), SIDE)),
            dma((len(NEAR), 2)), dma((len(NEAR), 2)),
            dma((SIDE,)), dma((SIDE,)), dma((SIDE,)), dma((SIDE,)),
            dma((ROWS,)), dma((ROWS,)), dma((ROWS,)), dma((ROWS,)),
            dma((ROWS,)), dma((ROWS,)),
            dma((OWNERS,)), dma((OWNERS,)),
        ],
        compiler_params=pltpu.CompilerParams(
            collective_id=0, has_side_effects=True, vmem_limit_bytes=36 << 20
        ),
    )(*(pltpu.with_memory_space_constraint(a, pltpu.HBM) for a in inputs))
    ready = jax.ShapeDtypeStruct((ROWS, rows, columns), BF16)
    ready_gate, ready_up, serve, scale_gate, scale_up = pl.pallas_call(
        lay_out,
        name="lay_out",
        out_shape=(ready, ready, router, scale, scale),
        in_specs=[vmem] * 4,
        out_specs=(hbm,) * 5,
        scratch_shapes=[dma((5,))],
        compiler_params=pltpu.CompilerParams(vmem_limit_bytes=8 << 20),
    )(*done)
    whole = (1, ROWS * rows, columns)
    return ready_gate.reshape(whole), ready_up.reshape(whole), scale_gate, scale_up, serve


def solution(mesh):
    return jax.shard_map(
        on_device,
        mesh=mesh,
        in_specs=(P("owner", "rows", None), P("owner", "rows", None), P("rows", "owner"), P("rows")),
        out_specs=(
            P(("owner", "rows"), None, None),
            P(("owner", "rows"), None, None),
            P(("owner", "rows"), None),
            P(("owner", "rows"), None),
            P(),
        ),
        check_vma=False,
    )
```
